32 devices in a mesh: row: 4 (over x, core), col: 8 (over z, y).
Axes of the slice: x: 2, y: 2, z: 4, core: 2. Of those that a mesh axis runs over, the one named last changes fastest.
Arguments:
- matrix: float32 [3072, 12, 4096], P('row', None, 'col'), may hold values from -6 to 6
- factor: float32 [12, 4096, 2048], P(None, 'col', 'row'), as said below
Outputs:
- updated: float32 [3072, 12, 4096], P('row', None, 'col')
- solved: float32 [3072, 2048], P('row')
The draws below stay inside these ranges and needn't reach their ends.
Inputs may be any that keep to these rules, and one draw needn't show every extreme that they name: factor is lower trapezoidal: zero wherever the column index exceeds the row index; its diagonal entries lie in 1 to 2.
All inputs are finite; a program needn't handle non-finite values.
Results may differ from the reference program's by a relative error of at most 0.00013.
Values sent between devices are 32-bit elements; how exact they have to be, the bound alone decides.
A program may use at most 256 MiB of HBM per device.

```python
import jax
import jax.numpy as jnp
from jax import lax

N = 49152
B = 512
P_SIZE = 4
M = 3072
LB = 12
N_COL = 8


def draw_factor(key, part):
    key_noise = jax.random.fold_in(key, 11)
    key_diag = jax.random.fold_in(key, 12)
    span = N // LB
    shape = (LB, span, P_SIZE * B)
    row_ids = jnp.arange(LB)[:, None, None] * span + jnp.arange(span)[None, :, None]
    col_ids = jnp.arange(P_SIZE * B)[None, None, :]
    noise = jax.random.normal(key_noise, shape, jnp.float32)
    same_block = row_ids // B == col_ids // B
    off_vals = jnp.where(same_block, 0.4, 1.0) * noise / jnp.sqrt(jnp.float32(B))
    diag_vals = jax.random.uniform(key_diag, shape, jnp.float32, 1.0, 2.0)
    lower_vals = jnp.where(row_ids > col_ids, off_vals, 0.0)
    return jnp.where(row_ids == col_ids, diag_vals, lower_vals).astype(jnp.float32)


def levels(own_key, shape, split, least, top_value):
    level = 1.0
    for axis_at, shards_of in split:
        heights = jax.random.uniform(jax.random.fold_in(jax.random.fold_in(own_key, 6), axis_at), (shards_of,), jnp.float32, least / len(split), top_value / len(split))
        level = level * jnp.repeat(jnp.exp(heights), shape[axis_at] // shards_of).reshape((-1,) + (1,) * (len(shape) - 1 - axis_at))
    return level


def bell_draw(stream_key, shape, spread, limit, shards=(), held_as=jnp.bfloat16):
    factor_of = levels(stream_key, shape, shards, -0.22, 0.18) if shards else 1.0
    values = jax.random.normal(stream_key, shape, jnp.float32) * spread * factor_of
    return jnp.minimum(jnp.maximum(values, -limit), limit).astype(held_as)


def setup_inputs(seed: int = 0) -> dict:
    seeds = jax.random.split(jax.random.key(seed), 3)
    return {
        "matrix": bell_draw(seeds[0], (M, LB, N_COL * B), 1.0, 6.0, ((0, 4), (2, 8)), jnp.float32),
        "factor": draw_factor(jax.random.fold_in(seeds[2], 71), 0),
    }


def reference(matrix, factor):
    row_count = matrix.shape[0]
    nblocks = N // B
    blocks = matrix.reshape(row_count, nblocks, B)
    factor_tiles = factor.reshape(nblocks, B, P_SIZE * B)
    panels = []
    for step in range(P_SIZE):
        right_side = blocks[:, step, :]
        if step > 0:
            earlier = jnp.concatenate(panels, axis=1)
            right_side = right_side - jnp.dot(earlier.astype(jnp.float32), factor_tiles[step, :, :step * B].T.astype(jnp.float32), precision=lax.Precision.HIGHEST, preferred_element_type=jnp.float32)
        diag_tile = factor_tiles[step, :, step * B:(step + 1) * B]
        solved_block = lax.linalg.triangular_solve(diag_tile, right_side, left_side=False, lower=True, transpose_a=True)
        panels.append(solved_block)
    solved = jnp.concatenate(panels, axis=1)
    block_of_row = (jnp.arange(N) // B).astype(jnp.int32)
    panel_of_col = (jnp.arange(P_SIZE * B) // B).astype(jnp.int32)
    active = panel_of_col[None, :] < block_of_row[:, None]
    masked = jnp.where(active, factor.reshape(N, P_SIZE * B), jnp.zeros((), factor.dtype))
    updated = matrix.reshape(row_count, N) - jnp.dot(solved.astype(jnp.float32), masked.T.astype(jnp.float32), precision=lax.Precision.HIGHEST, preferred_element_type=jnp.float32)
    return (updated.reshape(matrix.shape), solved)
```

```python
import jax
import jax.numpy as jnp
from jax import lax
from jax.experimental import pallas as pl
from jax.experimental.pallas import tpu as pltpu
from jax.sharding import PartitionSpec as P

ROW_PARTS = 2
CHUNK = 3
LEAF = 128


def dot_exact(a, b):
    return jnp.dot(a, b, precision=lax.Precision.HIGHEST, preferred_element_type=jnp.float32)


def invert_kernel(tile_ref, out_ref):
    width = tile_ref.shape[0]
    leaf = min(LEAF, width)
    rows = lax.broadcasted_iota(jnp.int32, (leaf, leaf), 0)
    cols = lax.broadcasted_iota(jnp.int32, (leaf, leaf), 1)
    on_diag = rows == cols
    out_ref[...] = jnp.zeros_like(out_ref)
    starts = range(0, width, leaf)
    tiles = [tile_ref[s : s + leaf, s : s + leaf] for s in starts]
    invs = [jnp.where(on_diag, 1.0 / jnp.where(on_diag, t, 1.0), 0.0) for t in tiles]
    shift = 0
    while (1 << shift) < leaf:
        below = ((rows >> (shift + 1)) == (cols >> (shift + 1))) & ((rows >> shift) > (cols >> shift))
        mids = [dot_exact(jnp.where(below, t, 0.0), v) for t, v in zip(tiles, invs)]
        invs = [v - dot_exact(v, m) for v, m in zip(invs, mids)]
        shift += 1
    for s, v in zip(starts, invs):
        out_ref[s : s + leaf, s : s + leaf] = v
    size = leaf
    while size < width:
        for s in range(0, width, 2 * size):
            mid = dot_exact(tile_ref[s + size : s + 2 * size, s : s + size], out_ref[s : s + size, s : s + size])
            out_ref[s + size : s + 2 * size, s : s + size] = -dot_exact(
                out_ref[s + size : s + 2 * size, s + size : s + 2 * size], mid
            )
        size *= 2


def invert(tile):
    return pl.pallas_call(
        invert_kernel,
        out_shape=jax.ShapeDtypeStruct(tile.shape, tile.dtype),
        in_specs=[pl.BlockSpec(memory_space=pltpu.VMEM)],
        out_specs=pl.BlockSpec(memory_space=pltpu.VMEM),
        cost_estimate=pl.CostEstimate(flops=12_000_000_000, bytes_accessed=2_000_000, transcendentals=0),
    )(tile)


def spread(value, root, group, count, index):
    holders = [root]
    rounds = []
    bit = 1
    while bit < group:
        rounds.append([(i, i ^ bit) for i in holders])
        holders = holders + [i ^ bit for i in holders]
        bit *= 2
    hop = max(group // 2, 1)
    for base in range(group, count, hop):
        rounds.append([(base - hop + j, base + j) for j in range(hop) if base + j < count])
    for pairs in rounds:
        got = lax.ppermute(value, "col", pairs)
        takes = jnp.zeros((), jnp.bool_)
        for _, to in pairs:
            takes = takes | (index == to)
        value = jnp.where(takes, got, value)
    return value


def local(matrix, factor):
    count = lax.axis_size("col")
    index = lax.axis_index("col")
    row_count, nlocal, width = matrix.shape
    panels = factor.shape[2] * lax.axis_size("row") // width
    assert panels <= count
    top = lax.all_gather(factor[0], "row", axis=1, tiled=True)
    top, later_factor = lax.optimization_barrier((top, factor))
    edges = [1]
    while edges[-1] < nlocal:
        edges.append(min(edges[-1] + CHUNK, nlocal))
    spans = list(zip(edges[:-1], edges[1:]))
    gathered = [lax.all_gather(later_factor[a:b], "row", axis=2, tiled=True) for a, b in spans]

    at = jnp.minimum(index, panels - 1) * width
    own_diag = lax.dynamic_slice(top, (0, at), (width, width))
    guarded = jnp.where(index < panels, own_diag, jnp.eye(width, dtype=jnp.float32))
    inverse = invert(guarded)

    part = row_count // ROW_PARTS
    current = [matrix[s * part : (s + 1) * part, 0, :] for s in range(ROW_PARTS)]
    solved_parts = [[] for _ in range(ROW_PARTS)]
    for step in range(panels):
        top_tile = top[:, step * width : (step + 1) * width]
        for s in range(ROW_PARTS):
            mine = jnp.einsum("ms,ts->mt", current[s], inverse, precision=lax.Precision.HIGHEST)
            x = spread(mine, step, panels, count, index)
            solved_parts[s].append(x)
            term = jnp.einsum("ms,ts->mt", x, top_tile, precision=lax.Precision.HIGHEST)
            current[s] = jnp.where(index > step, current[s] - term, current[s])
    solved = jnp.concatenate([jnp.concatenate(p, axis=1) for p in solved_parts], axis=0)
    pieces = [jnp.concatenate(current, axis=0)[:, None, :]]
    for (a, b), rows in zip(spans, gathered):
        term = jnp.einsum("ms,lts->mlt", solved, rows, precision=lax.Precision.HIGH)
        pieces.append(matrix[:, a:b, :] - term)
    return (jnp.concatenate(pieces, axis=1), solved)


def solution(mesh):
    return jax.shard_map(
        local,
        mesh=mesh,
        in_specs=(P("row", None, "col"), P(None, "col", "row")),
        out_specs=(P("row", None, "col"), P("row", None)),
        check_vma=False,
    )
```
